16 devices in a mesh: rep: 2 (over z), shard: 8 (over y, x, core).
Axes of the slice: x: 2, y: 2, z: 2, core: 2. Of those that a mesh axis runs over, the one named last changes fastest.
Arguments:
- x: bfloat16 [24576, 1536], P(('rep', 'shard'))
- seg_ids: int32 [24576], P(('rep', 'shard'))
- positions: int32 [24576], P(('rep', 'shard'))
- grad_y: bfloat16 [24576, 1536], P(('rep', 'shard'))
- num_tokens: int32 [1], replicated
- w_q: bfloat16 [1536, 1536], P('shard')
- b_q: bfloat16 [1536], P('shard')
- w_k: bfloat16 [1536, 256], P('shard')
- b_k: bfloat16 [256], P('shard')
- w_v: bfloat16 [1536, 256], P('shard')
- b_v: bfloat16 [256], P('shard')
- w_o: bfloat16 [1536, 1536], P('shard')
- w_gate: bfloat16 [1536, 8960], P('shard')
- w_up: bfloat16 [1536, 8960], P('shard')
- w_down: bfloat16 [8960, 1536], P('shard')
- norm_attn: bfloat16 [1536], P('shard')
- norm_mlp: bfloat16 [1536], P('shard')
Outputs:
- output 1: bfloat16 [24576, 1536], P(('rep', 'shard'))
- output 2: float32 [1536, 1536], P('shard')
- output 3: float32 [1536], P('shard')
- output 4: float32 [1536, 256], P('shard')
- output 5: float32 [256], P('shard')
- output 6: float32 [1536, 256], P('shard')
- output 7: float32 [256], P('shard')
- output 8: float32 [1536, 1536], P('shard')
- output 9: float32 [1536, 8960], P('shard')
- output 10: float32 [1536, 8960], P('shard')
- output 11: float32 [8960, 1536], P('shard')
- output 12: float32 [1536], P('shard')
- output 13: float32 [1536], P('shard')
All inputs are finite; a program needn't handle non-finite values.
Results may differ from the reference program's by a relative error of at most 0.02.
Values are sent between devices in bfloat16 or wider.
A program may use at most 1 GiB of HBM per device.

```python
import jax
import jax.numpy as jnp
from jax import lax

D = 1536
HEADS = 12
KV_HEADS = 2
HEAD = 128
FF = 8960
TOKENS = 1536
DEVICES = 16
QUERY_BLOCK = 128
NSEG = 2 + TOKENS // 1024
GROUP = HEADS // KV_HEADS
ROPE_THETA = 1000000.0
EPS = 1e-6


def draw_segments(seg_key):
    base_len = TOKENS // (2 * NSEG)
    spare_len = TOKENS - base_len * NSEG
    cut_points = jnp.sort(jax.random.randint(seg_key, (DEVICES, NSEG - 1), 0, spare_len + 1, dtype=jnp.int32), axis=-1)
    zero_col = jnp.zeros((DEVICES, 1), jnp.int32)
    spare_col = jnp.full((DEVICES, 1), spare_len, jnp.int32)
    bounds = jnp.concatenate([zero_col, cut_points, spare_col], axis=-1)
    lengths = base_len + bounds[:, 1:] - bounds[:, :-1]
    seg_ends = jnp.cumsum(lengths, axis=-1)[:, :-1]
    tok_ids = jnp.arange(TOKENS, dtype=jnp.int32)
    passed = tok_ids[None, :, None] >= seg_ends[:, None, :]
    seg_ids = jnp.sum(passed.astype(jnp.int32), axis=-1)
    starts = jnp.max(jnp.where(passed, seg_ends[:, None, :], 0), axis=-1)
    positions = tok_ids[None, :] - starts
    return seg_ids.reshape(DEVICES * TOKENS), positions.reshape(DEVICES * TOKENS)


def setup_inputs(seed: int = 0) -> dict:
    sub_keys = jax.random.split(jax.random.key(seed), 17)
    rows_all = DEVICES * TOKENS

    def normal_bf(idx, shape, scale):
        return (jax.random.normal(sub_keys[idx], shape, jnp.float32) * scale).astype(jnp.bfloat16)

    def gain_bf(idx):
        return (1.0 + 0.3 * jax.random.normal(sub_keys[idx], (D,), jnp.float32)).astype(jnp.bfloat16)

    seg_ids, positions = draw_segments(sub_keys[16])
    num_tokens = jax.random.randint(sub_keys[15], (1,), rows_all // 2, rows_all + 1, dtype=jnp.int32)
    return {
        'x': normal_bf(0, (rows_all, D), 1.0),
        'seg_ids': seg_ids,
        'positions': positions,
        'grad_y': normal_bf(1, (rows_all, D), 1.0),
        'num_tokens': num_tokens,
        'w_q': normal_bf(2, (D, HEADS * HEAD), D ** -0.5),
        'b_q': normal_bf(3, (HEADS * HEAD,), 0.5),
        'w_k': normal_bf(4, (D, KV_HEADS * HEAD), D ** -0.5),
        'b_k': normal_bf(5, (KV_HEADS * HEAD,), 0.5),
        'w_v': normal_bf(6, (D, KV_HEADS * HEAD), D ** -0.5),
        'b_v': normal_bf(7, (KV_HEADS * HEAD,), 0.5),
        'w_o': normal_bf(8, (HEADS * HEAD, D), (HEADS * HEAD) ** -0.5),
        'w_gate': normal_bf(9, (D, FF), D ** -0.5),
        'w_up': normal_bf(10, (D, FF), D ** -0.5),
        'w_down': normal_bf(11, (FF, D), FF ** -0.5),
        'norm_attn': gain_bf(12),
        'norm_mlp': gain_bf(13),
    }


def bf_round(vals):
    return vals.astype(jnp.bfloat16).astype(jnp.float32)


def rms_norm(vals, gain):
    return vals * lax.rsqrt(jnp.mean(vals * vals, axis=-1, keepdims=True) + EPS) * gain


def rope_tables(pos_blk):
    half_dim = HEAD // 2
    inv_freq = ROPE_THETA ** (-2.0 * jnp.arange(half_dim, dtype=jnp.float32) / HEAD)
    angle = pos_blk.astype(jnp.float32)[:, None] * inv_freq[None, :]
    cos_t = jnp.cos(angle)
    sin_t = jnp.sin(angle)
    return (jnp.concatenate([cos_t, cos_t], axis=-1)[:, None, :], jnp.concatenate([sin_t, sin_t], axis=-1)[:, None, :])


def rotate_half(vals):
    half_dim = vals.shape[-1] // 2
    return jnp.concatenate([-vals[..., half_dim:], vals[..., :half_dim]], axis=-1)


def rope_apply(vals, cos_t, sin_t):
    return vals * cos_t + rotate_half(vals) * sin_t


def attention(q_rot, k_rot, v_all, seg_blk):
    n_blocks = TOKENS // QUERY_BLOCK
    key_ids = jnp.arange(TOKENS)

    def one_block(block_in):
        q_blk, row_ids, seg_rows = block_in
        scores = jnp.einsum('qkgd,skd->kgqs', q_blk, k_rot) * (HEAD ** -0.5)
        allowed = (seg_rows[:, None] == seg_blk[None, :]) & (row_ids[:, None] >= key_ids[None, :])
        prob_vals = bf_round(jax.nn.softmax(jnp.where(allowed, scores, -1e30), axis=-1))
        return bf_round(jnp.einsum('kgqs,skd->qkgd', prob_vals, v_all))

    out_blocks = lax.map(jax.checkpoint(one_block), (q_rot.reshape(n_blocks, QUERY_BLOCK, KV_HEADS, GROUP, HEAD), key_ids.reshape(n_blocks, QUERY_BLOCK), seg_blk.reshape(n_blocks, QUERY_BLOCK)))
    return out_blocks.reshape(TOKENS, HEADS * HEAD)


def block_forward(x_blk, seg_blk, pos_blk, params):
    (w_q, b_q, w_k, b_k, w_v, b_v, w_o, w_gate, w_up, w_down, norm_attn, norm_mlp) = params
    normed_in = bf_round(rms_norm(x_blk, norm_attn))
    cos_t, sin_t = rope_tables(pos_blk)
    q_lin = jnp.dot(normed_in, w_q) + b_q
    k_lin = jnp.dot(normed_in, w_k) + b_k
    v_lin = jnp.dot(normed_in, w_v) + b_v
    q_rot = bf_round(rope_apply(q_lin.reshape(TOKENS, HEADS, HEAD), cos_t, sin_t))
    k_rot = bf_round(rope_apply(k_lin.reshape(TOKENS, KV_HEADS, HEAD), cos_t, sin_t))
    v_all = bf_round(v_lin).reshape(TOKENS, KV_HEADS, HEAD)
    attn_out = attention(q_rot.reshape(TOKENS, KV_HEADS, GROUP, HEAD), k_rot, v_all, seg_blk)
    resid = bf_round(x_blk + jnp.dot(attn_out, w_o))
    normed_mid = bf_round(rms_norm(resid, norm_mlp))
    hidden = bf_round(jax.nn.silu(jnp.dot(normed_mid, w_gate)) * jnp.dot(normed_mid, w_up))
    return resid + jnp.dot(hidden, w_down)


def reference(x, seg_ids, positions, grad_y, num_tokens, w_q, b_q, w_k, b_k, w_v, b_v, w_o, w_gate, w_up, w_down, norm_attn, norm_mlp):
    params = tuple(p.astype(jnp.float32) for p in (w_q, b_q, w_k, b_k, w_v, b_v, w_o, w_gate, w_up, w_down, norm_attn, norm_mlp))
    x_blocks = x.reshape(DEVICES, TOKENS, D)
    gy_blocks = grad_y.reshape(DEVICES, TOKENS, D)
    seg_blocks = seg_ids.reshape(DEVICES, TOKENS)
    pos_blocks = positions.reshape(DEVICES, TOKENS)

    def step(grad_sums, block_in):
        x_blk, seg_blk, pos_blk, gy_blk = block_in

        def layer_of(x_in, param_in):
            return block_forward(x_in, seg_blk, pos_blk, param_in)

        _, back_fn = jax.vjp(layer_of, x_blk.astype(jnp.float32), params)
        grad_x_blk, grad_params = back_fn(gy_blk.astype(jnp.float32))
        new_sums = jax.tree.map(jnp.add, grad_sums, grad_params)
        return new_sums, grad_x_blk.astype(jnp.bfloat16)

    zero_sums = tuple(jnp.zeros_like(p) for p in params)
    grad_sums, grad_x = lax.scan(step, zero_sums, (x_blocks, seg_blocks, pos_blocks, gy_blocks))
    inv_count = 1.0 / num_tokens[0].astype(jnp.float32)
    return (grad_x.reshape(DEVICES * TOKENS, D), grad_sums[0] * inv_count, grad_sums[1] * inv_count, grad_sums[2] * inv_count, grad_sums[3] * inv_count, grad_sums[4] * inv_count, grad_sums[5] * inv_count, grad_sums[6] * inv_count, grad_sums[7] * inv_count, grad_sums[8] * inv_count, grad_sums[9] * inv_count, grad_sums[10] * inv_count, grad_sums[11] * inv_count)
```

```python
import jax
import jax.numpy as jnp
from jax import lax
from jax.experimental import pallas as pl
from jax.experimental.pallas import tpu as pltpu
from jax.sharding import PartitionSpec as P


HEAD_DIM = 128
HEADS = 12
KV_HEADS = 2
GROUP = HEADS // KV_HEADS
ROPE_THETA = 1000000.0
EPS = 1e-6
QB = 256
SCALE = HEAD_DIM ** -0.5


def rope_tables(positions):
    half_dim = HEAD_DIM // 2
    inv_freq = ROPE_THETA ** (-2.0 * jnp.arange(half_dim, dtype=jnp.float32) / HEAD_DIM)
    angle = positions.astype(jnp.float32)[:, None] * inv_freq[None, :]
    cos_t = jnp.cos(angle)
    sin_t = jnp.sin(angle)
    return jnp.concatenate([cos_t, cos_t], axis=-1), jnp.concatenate([-sin_t, sin_t], axis=-1)


def dot_nn(a, b):
    return lax.dot_general(a, b, (((1,), (0,)), ((), ())), preferred_element_type=jnp.float32)


def dot_nt(a, b):
    return lax.dot_general(a, b, (((1,), (1,)), ((), ())), preferred_element_type=jnp.float32)


def dot_tn(a, b):
    return lax.dot_general(a, b, (((0,), (0,)), ((), ())), preferred_element_type=jnp.float32)


def round_bf(vals):
    return lax.reduce_precision(vals, 8, 7)


def masked_scores(k_part, q_blk, first_row, start_row):
    s_t = dot_nt(k_part, q_blk) * SCALE
    key_idx = lax.broadcasted_iota(jnp.int32, s_t.shape, 0)
    row_idx = lax.broadcasted_iota(jnp.int32, s_t.shape, 1) + first_row
    return jnp.where((key_idx >= start_row) & (key_idx <= row_idx), s_t, -1e30)


def attn_fwd_kernel(q_in, k_in, v_in, cos_ref, sin_ref, start_ref, q_out, k_out, v_out, o_out, vt_scr):
    tokens = q_in.shape[0]

    @pl.when(pl.program_id(0) % GROUP == 0)
    def _():
        k_f = k_in[...]
        k_out[...] = (k_f * cos_ref[...] + pltpu.roll(k_f, HEAD_DIM // 2, 1) * sin_ref[...]).astype(jnp.bfloat16)
        v_f = v_in[...]
        v_out[...] = v_f.astype(jnp.bfloat16)
        vt_scr[...] = v_f.T.astype(jnp.bfloat16)

    q_f = q_in[...]
    q_out[...] = (q_f * cos_ref[...] + pltpu.roll(q_f, HEAD_DIM // 2, 1) * sin_ref[...]).astype(jnp.bfloat16)
    for first in range(0, tokens, QB):
        keys = first + QB
        s_t = masked_scores(k_out[:keys, :], q_out[first:keys, :], first, start_ref[0:1, first:keys])
        e_t = jnp.exp(s_t - jnp.max(s_t, axis=0, keepdims=True))
        p_t = (e_t / jnp.sum(e_t, axis=0, keepdims=True)).astype(jnp.bfloat16)
        o_t = dot_nn(vt_scr[:, :keys], p_t)
        o_out[first:keys, :] = o_t.T.astype(jnp.bfloat16)


def column_sums(vals):
    return jnp.broadcast_to(jnp.sum(vals, axis=0, keepdims=True), (8, vals.shape[1]))


def attn_bwd_kernel(q_ref, k_ref, v_ref, do_ref, cos_ref, sin_ref, start_ref, dq_out, dk_out, dv_out, bq_out, bk_out, bv_out, dk_acc, dv_acc, kt_scr, dq_scr):
    tokens = q_ref.shape[0]
    step = pl.program_id(0) % GROUP

    @pl.when(step == 0)
    def _():
        kt_scr[...] = k_ref[...].astype(jnp.float32).T.astype(jnp.bfloat16)
        dk_acc[...] = jnp.zeros_like(dk_acc)
        dv_acc[...] = jnp.zeros_like(dv_acc)

    for first in range(0, tokens, QB):
        keys = first + QB
        q_blk = q_ref[first:keys, :]
        do_blk = do_ref[first:keys, :]
        s_t = masked_scores(k_ref[:keys, :], q_blk, first, start_ref[0:1, first:keys])
        e_t = jnp.exp(s_t - jnp.max(s_t, axis=0, keepdims=True))
        p_t = e_t / jnp.sum(e_t, axis=0, keepdims=True)
        dp_t = dot_nt(v_ref[:keys, :], do_blk)
        dv_acc[:keys, :] += dot_nn(p_t.astype(jnp.bfloat16), do_blk)
        delta = jnp.sum(p_t * dp_t, axis=0, keepdims=True)
        ds_t = (p_t * (dp_t - delta) * SCALE).astype(jnp.bfloat16)
        dk_acc[:keys, :] += dot_nn(ds_t, q_blk)
        dq_scr[first:keys, :] = dot_nn(kt_scr[:, :keys], ds_t).T

    def rope_back(grad):
        grad = grad.astype(jnp.bfloat16).astype(jnp.float32)
        return grad * cos_ref[...] - pltpu.roll(grad, HEAD_DIM // 2, 1) * sin_ref[...]

    dq_lin = rope_back(dq_scr[...])
    dq_out[...] = dq_lin.astype(jnp.bfloat16)
    bq_out[...] = column_sums(dq_lin)

    @pl.when(step == GROUP - 1)
    def _():
        dk_lin = rope_back(dk_acc[...])
        dk_out[...] = dk_lin.astype(jnp.bfloat16)
        bk_out[...] = column_sums(dk_lin)
        dv_bf = dv_acc[...].astype(jnp.bfloat16)
        dv_out[...] = dv_bf
        bv_out[...] = column_sums(dv_bf.astype(jnp.float32))


def head_spec(tokens, base):
    return pl.BlockSpec((tokens, HEAD_DIM), lambda h: (0, base + h))


def kv_spec(tokens, base):
    return pl.BlockSpec((tokens, HEAD_DIM), lambda h: (0, base + h // GROUP))


def whole_spec(shape):
    return pl.BlockSpec(shape, lambda h: (0, 0))


def attention_fwd(qkv_lin, cos_t, sin_t, start_row):
    tokens = qkv_lin.shape[0]
    table = whole_spec((tokens, HEAD_DIM))
    pairs = HEADS * tokens * tokens * 0.6
    return pl.pallas_call(
        attn_fwd_kernel,
        grid=(HEADS,),
        in_specs=[head_spec(tokens, 0), kv_spec(tokens, HEADS), kv_spec(tokens, HEADS + KV_HEADS), table, table, whole_spec((8, tokens))],
        out_specs=[head_spec(tokens, 0), kv_spec(tokens, 0), kv_spec(tokens, 0), head_spec(tokens, 0)],
        out_shape=[
            jax.ShapeDtypeStruct((tokens, HEADS * HEAD_DIM), jnp.bfloat16),
            jax.ShapeDtypeStruct((tokens, KV_HEADS * HEAD_DIM), jnp.bfloat16),
            jax.ShapeDtypeStruct((tokens, KV_HEADS * HEAD_DIM), jnp.bfloat16),
            jax.ShapeDtypeStruct((tokens, HEADS * HEAD_DIM), jnp.bfloat16),
        ],
        scratch_shapes=[pltpu.VMEM((HEAD_DIM, tokens), jnp.bfloat16)],
        compiler_params=pltpu.CompilerParams(dimension_semantics=("arbitrary",), vmem_limit_bytes=48 * 1024 * 1024),
        cost_estimate=pl.CostEstimate(flops=int(pairs * 128 * 16), bytes_accessed=30000000, transcendentals=int(pairs)),
        name="attn_fwd",
    )(qkv_lin, qkv_lin, qkv_lin, cos_t, sin_t, start_row)


def attention_bwd(q_rot, k_rot, v_all, d_out, cos_t, sin_t, start_row):
    tokens = q_rot.shape[0]
    table = whole_spec((tokens, HEAD_DIM))
    pairs = HEADS * tokens * tokens * 0.6
    row_q = pl.BlockSpec((8, HEAD_DIM), lambda h: (0, h))
    row_kv = pl.BlockSpec((8, HEAD_DIM), lambda h: (0, h // GROUP))
    acc = pltpu.VMEM((tokens, HEAD_DIM), jnp.float32)
    q_cols = HEADS * HEAD_DIM
    kv_cols = KV_HEADS * HEAD_DIM
    return pl.pallas_call(
        attn_bwd_kernel,
        grid=(HEADS,),
        in_specs=[head_spec(tokens, 0), kv_spec(tokens, 0), kv_spec(tokens, 0), head_spec(tokens, 0), table, table, whole_spec((8, tokens))],
        out_specs=[head_spec(tokens, 0), kv_spec(tokens, 0), kv_spec(tokens, 0), row_q, row_kv, row_kv],
        out_shape=[
            jax.ShapeDtypeStruct((tokens, q_cols), jnp.bfloat16),
            jax.ShapeDtypeStruct((tokens, kv_cols), jnp.bfloat16),
            jax.ShapeDtypeStruct((tokens, kv_cols), jnp.bfloat16),
            jax.ShapeDtypeStruct((8, q_cols), jnp.float32),
            jax.ShapeDtypeStruct((8, kv_cols), jnp.float32),
            jax.ShapeDtypeStruct((8, kv_cols), jnp.float32),
        ],
        scratch_shapes=[acc, acc, pltpu.VMEM((HEAD_DIM, tokens), jnp.bfloat16), acc],
        compiler_params=pltpu.CompilerParams(dimension_semantics=("arbitrary",), vmem_limit_bytes=48 * 1024 * 1024),
        cost_estimate=pl.CostEstimate(flops=int(pairs * 128 * 30), bytes_accessed=30000000, transcendentals=int(pairs)),
        name="attn_bwd",
    )(q_rot, k_rot, v_all, d_out, cos_t, sin_t, start_row)


def rms_inverse(vals):
    return lax.rsqrt(jnp.mean(vals * vals, axis=-1, keepdims=True) + EPS)


def rms_back(d_normed, vals, inv_rms, gain):
    d_scaled = d_normed * gain
    d_vals = inv_rms * d_scaled - vals * (inv_rms ** 3) * jnp.mean(d_scaled * vals, axis=-1, keepdims=True)
    return d_vals, jnp.sum(d_normed * vals * inv_rms, axis=0)


def pick(arr, index, axis):
    return lax.dynamic_index_in_dim(arr, index, axis, keepdims=False)


def swap(arr, bit):
    return lax.ppermute(arr, 'shard', [(s, s ^ bit) for s in range(8)])


def swap_rep(arr):
    return lax.ppermute(arr, 'rep', [(0, 1), (1, 0)])


def f32(arr):
    return arr.astype(jnp.float32)


def bf16(arr):
    return arr.astype(jnp.bfloat16)


def stack_rows(vecs):
    rows = [jnp.pad(v, [(0, 0)] * (v.ndim - 1) + [(0, 256 - v.shape[-1])]) for v in vecs]
    rows = jnp.concatenate(rows, axis=-2)
    return jnp.pad(rows, [(0, 0)] * (rows.ndim - 2) + [(0, 8 - len(vecs)), (0, 0)])


class Spot:
    def __init__(self):
        shard = lax.axis_index('shard')
        self.core = shard % 2
        self.x = (shard // 2) % 2
        self.y = shard // 4


def split_rows(spot, acts, rows):
    tokens = acts.shape[0]
    cut = acts.T.reshape(2, 2, 2, rows, tokens)
    to_core = pick(cut, 1 - spot.core, 2).reshape(4 * rows, tokens)
    mine = pick(cut, spot.core, 2)
    x_send = pick(mine, 1 - spot.x, 1).reshape(2 * rows, tokens)
    x_keep = pick(mine, spot.x, 1).reshape(2 * rows, tokens)
    y_send = pick(mine, 1 - spot.y, 0).reshape(2 * rows, tokens)
    y_keep = pick(mine, spot.y, 0).reshape(2 * rows, tokens)
    return to_core, (x_send, x_keep), (y_send, y_keep)


def tie(now, after):
    out = lax.optimization_barrier((tuple(now), tuple(after)))
    return out[0]


class WeightSum:
    def __init__(self, spot, parts, x_first, rows):
        self.spot, self.x_first, self.rows = spot, x_first, rows
        self.to_core = parts[0]
        self.send_acts, self.keep_acts = parts[1] if x_first else parts[2]
        self.axis, self.here, self.bit = (1, spot.x, 2) if x_first else (0, spot.y, 4)
        self.here2, self.bit2 = (spot.y, 4) if x_first else (spot.x, 2)

    def core(self, grads):
        self.sent = bf16(dot_nn(self.to_core, grads))
        self.got = swap(self.sent, 1)
        return self.sent

    def first(self, got, grads):
        cols = grads.shape[1]
        got = got.reshape(2, 2, self.rows, cols)
        got_send = pick(got, 1 - self.here, self.axis).reshape(2 * self.rows, cols)
        got_keep = pick(got, self.here, self.axis).reshape(2 * self.rows, cols)
        self.sent = bf16(dot_nn(self.send_acts, grads) + f32(got_send))
        self.got = swap(self.sent, self.bit)
        self.kept = dot_nn(self.keep_acts, grads) + f32(got_keep)
        return self.kept

    def second(self, got, kept):
        cols = got.shape[1]
        got = got.reshape(2, self.rows, cols)
        kept = kept.reshape(2, self.rows, cols)
        self.sent = bf16(pick(kept, 1 - self.here2, 0) + f32(pick(got, 1 - self.here2, 0)))
        self.got = swap(self.sent, self.bit2)
        self.kept = pick(kept, self.here2, 0) + f32(pick(got, self.here2, 0))
        return self.sent

    def third(self, got, kept):
        self.sent = bf16(kept + f32(got))
        self.got = swap_rep(self.sent)
        return self.sent

    def result(self):
        return f32(self.sent) + f32(self.got)


def solution(mesh):
    batch_spec = P(('rep', 'shard'), None)
    row_spec = P(('rep', 'shard'))
    mat_spec = P('shard', None)
    vec_spec = P('shard')
    weight_specs = (mat_spec, vec_spec, mat_spec, vec_spec, mat_spec, vec_spec, mat_spec, mat_spec, mat_spec, mat_spec, vec_spec, vec_spec)
    in_specs = (batch_spec, row_spec, row_spec, batch_spec, P(None)) + weight_specs
    out_specs = (batch_spec,) + weight_specs

    def gather(part):
        return lax.all_gather(part, 'shard', axis=0, tiled=True)

    def per_device(x, seg_ids, positions, grad_y, num_tokens, w_q, b_q, w_k, b_k, w_v, b_v, w_o, w_gate, w_up, w_down, norm_attn, norm_mlp):
        tokens, width = x.shape
        ff = w_gate.shape[1]
        half = ff // 2
        q_cols, kv_cols = w_q.shape[1], w_k.shape[1]
        rows = w_q.shape[0]
        down_rows = w_down.shape[0]
        spot = Spot()
        inv_count = 1.0 / num_tokens[0].astype(jnp.float32)

        wqkv = gather(jnp.concatenate([w_q, w_k, w_v], axis=1))
        small_list = [b_q, b_k, b_v, norm_attn, norm_mlp]
        sizes = [v.shape[0] for v in small_list]
        small = lax.all_gather(stack_rows([f32(v)[None, :] for v in small_list]), 'shard', axis=0, tiled=False)
        wo = gather(w_o)
        wg0 = gather(w_gate[:, :half])
        wu0 = gather(w_up[:, :half])
        wdown = gather(w_down)
        wg1 = gather(w_gate[:, half:])
        wu1 = gather(w_up[:, half:])

        cuts = [small[:, i, :n].reshape(-1) for i, n in enumerate(sizes)]
        bias = jnp.concatenate(cuts[:3])
        gain_in, gain_mid = cuts[3], cuts[4]

        cos_t, sin_t = rope_tables(positions)
        start_row = jnp.broadcast_to((jnp.arange(tokens, dtype=jnp.int32) - positions)[None, :], (8, tokens))
        x_f = f32(x)
        inv_in = rms_inverse(x_f)
        normed_in = bf16(x_f * inv_in * gain_in)
        qkv_lin = dot_nn(normed_in, wqkv) + bias
        q_rot, k_rot, v_all, attn_out = attention_fwd(qkv_lin, cos_t, sin_t, start_row)
        resid = bf16(x_f + dot_nn(attn_out, wo))
        resid_f = f32(resid)
        inv_mid = rms_inverse(resid_f)
        normed_mid = bf16(resid_f * inv_mid * gain_mid)

        mid_parts = split_rows(spot, normed_mid, rows)
        o_parts = split_rows(spot, attn_out, rows)
        in_parts = split_rows(spot, normed_in, rows)
        flat_parts = jax.tree.leaves((mid_parts, o_parts, in_parts))

        def swiglu_back(gate_pre, up_proj, d_hid):
            sig_gate = jax.nn.sigmoid(gate_pre)
            act_gate = gate_pre * sig_gate
            d_gate = bf16(d_hid * up_proj * sig_gate * (1.0 + gate_pre * (1.0 - sig_gate)))
            return d_gate, bf16(d_hid * act_gate)

        def down_core(hidden):
            full = dot_tn(hidden, grad_y).reshape(2, 2, down_rows, width)
            return full, swap(bf16(pick(full, 1 - spot.core, 1)), 1)

        def down_x(full, got):
            mine = pick(full, spot.core, 1)
            sent = bf16(pick(mine, 1 - spot.x, 0) + f32(pick(got, 1 - spot.x, 0)))
            return sent, pick(mine, spot.x, 0) + f32(pick(got, spot.x, 0)), swap(sent, 2)

        n_mid, *flat_parts = tie([normed_mid] + flat_parts, [resid])
        mid_parts, o_parts, in_parts = jax.tree.unflatten(jax.tree.structure((mid_parts, o_parts, in_parts)), flat_parts)
        gate_sums = [WeightSum(spot, mid_parts, True, rows) for _ in range(2)]
        up_sums = [WeightSum(spot, mid_parts, False, rows) for _ in range(2)]

        gate0 = dot_nn(n_mid, wg0)
        up0 = dot_nn(n_mid, wu0)
        hidden0 = bf16(gate0 * jax.nn.sigmoid(gate0) * up0)
        hidden0, gate0, up0 = tie([hidden0, gate0, up0], [])
        full0, dgot0 = down_core(hidden0)
        d_hid0 = dot_nt(grad_y, tie([wdown], [full0])[0][:half])
        dg0, du0 = swiglu_back(gate0, up0, round_bf(d_hid0))

        dg0, du0, dgot0, full0 = tie([dg0, du0, dgot0, full0], [])
        dsent0, dkept0, dgot0x = down_x(full0, dgot0)
        c_g0 = gate_sums[0].core(dg0)
        c_u0 = up_sums[0].core(du0)
        dg0, du0, wg0b, wu0b = tie([dg0, du0, wg0, wu0], [c_g0, c_u0, dsent0, dkept0])
        d_mid = dot_nt(dg0, wg0b) + dot_nt(du0, wu0b)
        dg0, du0, got_g, got_u, n_mid = tie([dg0, du0, gate_sums[0].got, up_sums[0].got, n_mid], [d_mid])
        k_g0 = gate_sums[0].first(got_g, dg0)
        k_u0 = up_sums[0].first(got_u, du0)

        n_mid, wd1 = tie([n_mid, wdown], [k_g0, k_u0, gate_sums[0].sent, up_sums[0].sent])
        gate1 = dot_nn(n_mid, wg1)
        d_hid1 = bf16(dot_nt(grad_y, wd1[half:]))
        gate1, d_hid1 = tie([gate1, d_hid1], [])
        n_mid, = tie([n_mid], [gate1, d_hid1])
        up1 = dot_nn(n_mid, wu1)
        hidden1 = bf16(gate1 * jax.nn.sigmoid(gate1) * up1)
        dg1, du1 = swiglu_back(gate1, up1, f32(d_hid1))
        hidden1, dg1, du1, k_g0, k_u0, got_g, got_u = tie([hidden1, dg1, du1, k_g0, k_u0, gate_sums[0].got, up_sums[0].got], [])
        s_g0 = gate_sums[0].second(got_g, k_g0)
        s_u0 = up_sums[0].second(got_u, k_u0)
        c_g1 = gate_sums[1].core(dg1)
        c_u1 = up_sums[1].core(du1)
        hidden1, = tie([hidden1], [c_g1, c_u1, s_g0, s_u0])
        full1, dgot1 = down_core(hidden1)
        dg1, du1, got_g, got_u, full1 = tie([dg1, du1, gate_sums[1].got, up_sums[1].got, full1], [])
        k_g1 = gate_sums[1].first(got_g, dg1)
        k_u1 = up_sums[1].first(got_u, du1)
        dg1, du1, dgot1, full1, k_g1, k_u1, got_g, got_u = tie([dg1, du1, dgot1, full1, k_g1, k_u1, gate_sums[0].got, up_sums[0].got], [gate_sums[1].sent, up_sums[1].sent])
        t_g0 = gate_sums[0].third(got_g, gate_sums[0].kept)
        t_u0 = up_sums[0].third(got_u, up_sums[0].kept)
        dsent1, dkept1, dgot1x = down_x(full1, dgot1)
        dg1, du1, d_mid = tie([dg1, du1, d_mid], [t_g0, t_u0, dsent1, dkept1])
        d_mid = round_bf(d_mid + dot_nt(dg1, wg1) + dot_nt(du1, wu1))

        d_resid_norm, sum_norm_mlp = rms_back(d_mid, resid_f, inv_mid, gain_mid)
        d_resid = bf16(f32(grad_y) + d_resid_norm)
        d_resid, dkept0, dkept1, dgot0x, k_g1, k_u1, got_g, got_u = tie([d_resid, dkept0, dkept1, dgot0x, k_g1, k_u1, gate_sums[1].got, up_sums[1].got], [])
        s_g1 = gate_sums[1].second(got_g, k_g1)
        s_u1 = up_sums[1].second(got_u, k_u1)
        o_cut = width // 2
        o_sums = [WeightSum(spot, o_parts, first, rows) for first in (True, False)]
        c_o = [o_sums[i].core(d_resid[:, i * o_cut:(i + 1) * o_cut]) for i in range(2)]
        d_res_m, dgot1x = tie([d_resid, dgot1x], c_o + [s_g1, s_u1])
        low = spot.y == 0
        down_sent = bf16(jnp.where(low, dkept1 + f32(dgot1x), dkept0 + f32(dgot0x)))
        down_kept = jnp.where(low, dkept0 + f32(dgot0x), dkept1 + f32(dgot1x))
        down_got = swap(down_sent, 4)
        d_attn = bf16(dot_nt(d_res_m, wo))
        d_attn, got_g, got_u, got_o0, got_o1 = tie([d_attn, gate_sums[1].got, up_sums[1].got, o_sums[0].got, o_sums[1].got], [down_sent, down_kept])
        k_o = [o_sums[i].first(got, d_resid[:, i * o_cut:(i + 1) * o_cut]) for i, got in enumerate((got_o0, got_o1))]
        t_g1 = gate_sums[1].third(got_g, gate_sums[1].kept)
        t_u1 = up_sums[1].third(got_u, up_sums[1].kept)
        d_attn, = tie([d_attn], k_o + [t_g1, t_u1, o_sums[0].sent, o_sums[1].sent])
        d_q, d_k, d_v, sum_bq, sum_bk, sum_bv = attention_bwd(q_rot, k_rot, v_all, d_attn, cos_t, sin_t, start_row)
        d_qkv = jnp.concatenate([d_q, d_k, d_v], axis=1)
        d_qkv, k_o0, k_o1, got_o0, got_o1, down_got, down_kept = tie([d_qkv] + k_o + [o_sums[0].got, o_sums[1].got, down_got, down_kept], [])
        s_o = [o_sums[0].second(got_o0, k_o0), o_sums[1].second(got_o1, k_o1)]
        down_mine = bf16(down_kept + f32(down_got))
        down_rep = swap_rep(down_mine)
        q_cut = d_qkv.shape[1] // 2
        q_sums = [WeightSum(spot, in_parts, first, rows) for first in (True, False)]
        c_q = [q_sums[i].core(d_qkv[:, i * q_cut:(i + 1) * q_cut]) for i in range(2)]
        d_qkv, got_q0, got_q1 = tie([d_qkv, q_sums[0].got, q_sums[1].got], s_o + c_q + [down_mine])
        k_q = [q_sums[i].first(got, d_qkv[:, i * q_cut:(i + 1) * q_cut]) for i, got in enumerate((got_q0, got_q1))]
        d_qkv, got_o0, got_o1 = tie([d_qkv, o_sums[0].got, o_sums[1].got], k_q + [q_sums[0].sent, q_sums[1].sent])
        t_o = [o_sums[0].third(got_o0, o_sums[0].kept), o_sums[1].third(got_o1, o_sums[1].kept)]
        d_qkv, = tie([d_qkv], t_o)
        d_normed_in = round_bf(dot_nt(d_qkv, wqkv))
        d_x_norm, sum_norm_attn = rms_back(d_normed_in, x_f, inv_in, gain_in)
        grad_x = bf16(f32(d_resid) + d_x_norm)
        k_q0, k_q1, got_q0, got_q1, grad_x, sum_norm_attn = tie(k_q + [q_sums[0].got, q_sums[1].got, grad_x, sum_norm_attn], [])
        s_q = [q_sums[0].second(got_q0, k_q0), q_sums[1].second(got_q1, k_q1)]
        sum_norm_attn, = tie([sum_norm_attn], s_q)

        vecs = [sum_bq[0], sum_bk[0], sum_bv[0], sum_norm_attn, sum_norm_mlp]
        flat = stack_rows([v.reshape(8, 1, -1) for v in vecs])
        flat = pick(lax.psum(flat, ('rep', 'shard')), lax.axis_index('shard'), 0) * inv_count
        vec_out = [flat[i, :n] for i, n in enumerate(sizes)]
        for part in q_sums:
            part.third(part.got, part.kept)

        def joined(parts):
            return jnp.concatenate([part.result() for part in parts], axis=1) * inv_count

        qkv_sum = joined(q_sums)
        return (grad_x, qkv_sum[:, :q_cols], vec_out[0], qkv_sum[:, q_cols:q_cols + kv_cols], vec_out[1], qkv_sum[:, q_cols + kv_cols:], vec_out[2], joined(o_sums),
                joined(gate_sums), joined(up_sums), (f32(down_mine) + f32(down_rep)) * inv_count, vec_out[3], vec_out[4])

    return jax.shard_map(per_device, mesh=mesh, in_specs=in_specs, out_specs=out_specs, check_vma=False)
```

```python
import jax
import jax.numpy as jnp
from jax import lax
from jax.experimental import pallas as pl
from jax.experimental.pallas import tpu as pltpu
from jax.sharding import PartitionSpec as P


HEAD_DIM = 128
HEADS = 12
KV_HEADS = 2
GROUP = HEADS // KV_HEADS
ROPE_THETA = 1000000.0
EPS = 1e-6
QB = 256
SCALE = HEAD_DIM ** -0.5
LOG2E = 1.4426950408889634


def rope_tables(positions):
    half_dim = HEAD_DIM // 2
    inv_freq = ROPE_THETA ** (-2.0 * jnp.arange(half_dim, dtype=jnp.float32) / HEAD_DIM)
    angle = positions.astype(jnp.float32)[:, None] * inv_freq[None, :]
    cos_t = jnp.cos(angle)
    sin_t = jnp.sin(angle)
    return jnp.concatenate([cos_t, cos_t], axis=-1), jnp.concatenate([-sin_t, sin_t], axis=-1)


def dot_nn(a, b):
    return lax.dot_general(a, b, (((1,), (0,)), ((), ())), preferred_element_type=jnp.float32)


def dot_nt(a, b):
    return lax.dot_general(a, b, (((1,), (1,)), ((), ())), preferred_element_type=jnp.float32)


def dot_tn(a, b):
    return lax.dot_general(a, b, (((0,), (0,)), ((), ())), preferred_element_type=jnp.float32)


def round_bf(vals):
    return lax.reduce_precision(vals, 8, 7)


def exp_scores(k_part, q_blk, first_row, start_row):
    s_t = dot_nt(k_part, q_blk)
    key_idx = lax.broadcasted_iota(jnp.int32, (QB, QB), 0)
    row_idx = lax.broadcasted_iota(jnp.int32, (QB, QB), 1)
    parts = []
    for base in range(0, first_row, QB):
        parts.append(jnp.where(key_idx >= start_row - base, s_t[base:base + QB], -1e30))
    parts.append(jnp.where((key_idx >= start_row - first_row) & (key_idx <= row_idx), s_t[first_row:], -1e30))
    s_t = jnp.concatenate(parts, axis=0)
    e_t = jnp.exp2((s_t - jnp.max(s_t, axis=0, keepdims=True)) * (SCALE * LOG2E))
    return e_t, 1.0 / jnp.sum(e_t, axis=0, keepdims=True)


def attn_fwd_kernel(q_in, k_in, v_in, cos_ref, sin_ref, start_ref, q_out, k_out, v_out, o_out, vt_scr):
    tokens = q_in.shape[0]

    @pl.when(pl.program_id(0) % GROUP == 0)
    def _():
        k_f = k_in[...]
        k_out[...] = (k_f * cos_ref[...] + pltpu.roll(k_f, HEAD_DIM // 2, 1) * sin_ref[...]).astype(jnp.bfloat16)
        v_f = v_in[...]
        v_out[...] = v_f.astype(jnp.bfloat16)
        vt_scr[...] = v_f.T.astype(jnp.bfloat16)

    q_f = q_in[...]
    q_out[...] = (q_f * cos_ref[...] + pltpu.roll(q_f, HEAD_DIM // 2, 1) * sin_ref[...]).astype(jnp.bfloat16)
    for first in range(0, tokens, QB):
        keys = first + QB
        e_t, inv_sum = exp_scores(k_out[:keys, :], q_out[first:keys, :], first, start_ref[0:1, first:keys])
        p_t = (e_t * inv_sum).astype(jnp.bfloat16)
        o_t = dot_nn(vt_scr[:, :keys], p_t)
        o_out[first:keys, :] = o_t.T.astype(jnp.bfloat16)


def column_sums(vals):
    return jnp.broadcast_to(jnp.sum(vals, axis=0, keepdims=True), (8, vals.shape[1]))


def attn_bwd_kernel(q_ref, k_ref, v_ref, do_ref, cos_ref, sin_ref, start_ref, dq_out, dk_out, dv_out, bq_out, bk_out, bv_out, dk_acc, dv_acc, kt_scr, dq_scr):
    tokens = q_ref.shape[0]
    step = pl.program_id(0) % GROUP

    @pl.when(step == 0)
    def _():
        kt_scr[...] = k_ref[...].astype(jnp.float32).T.astype(jnp.bfloat16)
        dk_acc[...] = jnp.zeros_like(dk_acc)
        dv_acc[...] = jnp.zeros_like(dv_acc)

    for first in range(0, tokens, QB):
        keys = first + QB
        q_blk = q_ref[first:keys, :]
        do_blk = do_ref[first:keys, :]
        e_t, inv_sum = exp_scores(k_ref[:keys, :], q_blk, first, start_ref[0:1, first:keys])
        p_t = e_t * inv_sum
        dp_t = dot_nt(v_ref[:keys, :], do_blk)
        dv_acc[:keys, :] += dot_nn(p_t.astype(jnp.bfloat16), do_blk)
        delta = jnp.sum(p_t * dp_t, axis=0, keepdims=True)
        ds_t = (p_t * (dp_t - delta) * SCALE).astype(jnp.bfloat16)
        dk_acc[:keys, :] += dot_nn(ds_t, q_blk)
        dq_scr[first:keys, :] = dot_nn(kt_scr[:, :keys], ds_t).T

    def rope_back(grad):
        grad = grad.astype(jnp.bfloat16).astype(jnp.float32)
        return grad * cos_ref[...] - pltpu.roll(grad, HEAD_DIM // 2, 1) * sin_ref[...]

    dq_lin = rope_back(dq_scr[...])
    dq_out[...] = dq_lin.astype(jnp.bfloat16)
    bq_out[...] = column_sums(dq_lin)

    @pl.when(step == GROUP - 1)
    def _():
        dk_lin = rope_back(dk_acc[...])
        dk_out[...] = dk_lin.astype(jnp.bfloat16)
        bk_out[...] = column_sums(dk_lin)
        dv_bf = dv_acc[...].astype(jnp.bfloat16)
        dv_out[...] = dv_bf
        bv_out[...] = column_sums(dv_bf.astype(jnp.float32))


def head_spec(tokens, base):
    return pl.BlockSpec((tokens, HEAD_DIM), lambda h: (0, base + h))


def kv_spec(tokens, base):
    return pl.BlockSpec((tokens, HEAD_DIM), lambda h: (0, base + h // GROUP))


def whole_spec(shape):
    return pl.BlockSpec(shape, lambda h: (0, 0))


def attention_fwd(qkv_lin, cos_t, sin_t, start_row):
    tokens = qkv_lin.shape[0]
    table = whole_spec((tokens, HEAD_DIM))
    pairs = HEADS * tokens * tokens * 0.6
    return pl.pallas_call(
        attn_fwd_kernel,
        grid=(HEADS,),
        in_specs=[head_spec(tokens, 0), kv_spec(tokens, HEADS), kv_spec(tokens, HEADS + KV_HEADS), table, table, whole_spec((8, tokens))],
        out_specs=[head_spec(tokens, 0), kv_spec(tokens, 0), kv_spec(tokens, 0), head_spec(tokens, 0)],
        out_shape=[
            jax.ShapeDtypeStruct((tokens, HEADS * HEAD_DIM), jnp.bfloat16),
            jax.ShapeDtypeStruct((tokens, KV_HEADS * HEAD_DIM), jnp.bfloat16),
            jax.ShapeDtypeStruct((tokens, KV_HEADS * HEAD_DIM), jnp.bfloat16),
            jax.ShapeDtypeStruct((tokens, HEADS * HEAD_DIM), jnp.bfloat16),
        ],
        scratch_shapes=[pltpu.VMEM((HEAD_DIM, tokens), jnp.bfloat16)],
        compiler_params=pltpu.CompilerParams(dimension_semantics=("arbitrary",), vmem_limit_bytes=48 * 1024 * 1024),
        cost_estimate=pl.CostEstimate(flops=int(pairs * 128 * 16), bytes_accessed=30000000, transcendentals=int(pairs)),
        name="attn_fwd",
    )(qkv_lin, qkv_lin, qkv_lin, cos_t, sin_t, start_row)


def attention_bwd(kv_head, q_rot, k_rot, v_all, d_out, cos_t, sin_t, start_row):
    tokens = q_rot.shape[0]
    table = whole_spec((tokens, HEAD_DIM))
    pairs = GROUP * tokens * tokens * 0.6
    q_in = head_spec(tokens, kv_head * GROUP)
    kv_in = pl.BlockSpec((tokens, HEAD_DIM), lambda h: (0, kv_head))
    row_q = pl.BlockSpec((8, HEAD_DIM), lambda h: (0, h))
    acc = pltpu.VMEM((tokens, HEAD_DIM), jnp.float32)
    q_cols = GROUP * HEAD_DIM
    return pl.pallas_call(
        attn_bwd_kernel,
        grid=(GROUP,),
        in_specs=[q_in, kv_in, kv_in, q_in, table, table, whole_spec((8, tokens))],
        out_specs=[head_spec(tokens, 0), table, table, row_q, whole_spec((8, HEAD_DIM)), whole_spec((8, HEAD_DIM))],
        out_shape=[
            jax.ShapeDtypeStruct((tokens, q_cols), jnp.bfloat16),
            jax.ShapeDtypeStruct((tokens, HEAD_DIM), jnp.bfloat16),
            jax.ShapeDtypeStruct((tokens, HEAD_DIM), jnp.bfloat16),
            jax.ShapeDtypeStruct((8, q_cols), jnp.float32),
            jax.ShapeDtypeStruct((8, HEAD_DIM), jnp.float32),
            jax.ShapeDtypeStruct((8, HEAD_DIM), jnp.float32),
        ],
        scratch_shapes=[acc, acc, pltpu.VMEM((HEAD_DIM, tokens), jnp.bfloat16), acc],
        compiler_params=pltpu.CompilerParams(dimension_semantics=("arbitrary",), vmem_limit_bytes=48 * 1024 * 1024),
        cost_estimate=pl.CostEstimate(flops=int(pairs * 128 * 30), bytes_accessed=15000000, transcendentals=int(pairs)),
        name="attn_bwd",
    )(q_rot, k_rot, v_all, d_out, cos_t, sin_t, start_row)


def rms_inverse(vals):
    return lax.rsqrt(jnp.mean(vals * vals, axis=-1, keepdims=True) + EPS)


def rms_back(d_normed, vals, inv_rms, gain):
    d_scaled = d_normed * gain
    d_vals = inv_rms * d_scaled - vals * (inv_rms ** 3) * jnp.mean(d_scaled * vals, axis=-1, keepdims=True)
    return d_vals, jnp.sum(d_normed * vals * inv_rms, axis=0)


def pick(arr, index, axis):
    return lax.dynamic_index_in_dim(arr, index, axis, keepdims=False)


def swap(arr, bit):
    return lax.ppermute(arr, 'shard', [(s, s ^ bit) for s in range(8)])


def swap_rep(arr):
    return lax.ppermute(arr, 'rep', [(0, 1), (1, 0)])


def f32(arr):
    return arr.astype(jnp.float32)


def bf16(arr):
    return arr.astype(jnp.bfloat16)


def stack_rows(vecs):
    rows = [jnp.pad(v, [(0, 0)] * (v.ndim - 1) + [(0, 256 - v.shape[-1])]) for v in vecs]
    rows = jnp.concatenate(rows, axis=-2)
    return jnp.pad(rows, [(0, 0)] * (rows.ndim - 2) + [(0, 8 - len(vecs)), (0, 0)])


class Spot:
    def __init__(self):
        shard = lax.axis_index('shard')
        self.core = shard % 2
        self.x = (shard // 2) % 2
        self.y = shard // 4


def split_rows(spot, acts, rows):
    tokens = acts.shape[0]
    cut = acts.T.reshape(2, 2, 2, rows, tokens)
    out = []
    for axis, here in ((1, spot.x), (0, spot.y)):
        pair = []
        for core in (1 - spot.core, spot.core):
            mine = pick(cut, core, 2)
            pair.append(jnp.stack([pick(mine, 1 - here, axis), pick(mine, here, axis)]).reshape(4 * rows, tokens))
        out.append(tuple(pair))
    return tuple(out)


def tie(now, after):
    out = lax.optimization_barrier((tuple(now), tuple(after)))
    return out[0]


class WeightSum:
    def __init__(self, spot, parts, x_first, rows):
        self.spot, self.x_first, self.rows = spot, x_first, rows
        self.to_core, self.own_acts = parts[0] if x_first else parts[1]
        self.bit = 2 if x_first else 4
        self.here2, self.bit2 = (spot.y, 4) if x_first else (spot.x, 2)

    def core(self, grads):
        self.sent = bf16(dot_nn(self.to_core, grads))
        self.got = swap(self.sent, 1)
        return self.sent

    def first(self, got, grads):
        own, = tie([dot_nn(self.own_acts, grads) + f32(got)], [])
        self.sent = bf16(own[:2 * self.rows])
        self.got = swap(self.sent, self.bit)
        self.kept = own[2 * self.rows:]
        return self.kept

    def second(self, got, kept):
        cols = got.shape[1]
        got = got.reshape(2, self.rows, cols)
        kept = kept.reshape(2, self.rows, cols)
        self.sent = bf16(pick(kept, 1 - self.here2, 0) + f32(pick(got, 1 - self.here2, 0)))
        self.got = swap(self.sent, self.bit2)
        self.kept = pick(kept, self.here2, 0) + f32(pick(got, self.here2, 0))
        return self.sent

    def third(self, got, kept):
        self.sent = bf16(kept + f32(got))
        self.got = swap_rep(self.sent)
        return self.sent

    def result(self):
        return f32(self.sent) + f32(self.got)


def solution(mesh):
    batch_spec = P(('rep', 'shard'), None)
    row_spec = P(('rep', 'shard'))
    mat_spec = P('shard', None)
    vec_spec = P('shard')
    weight_specs = (mat_spec, vec_spec, mat_spec, vec_spec, mat_spec, vec_spec, mat_spec, mat_spec, mat_spec, mat_spec, vec_spec, vec_spec)
    in_specs = (batch_spec, row_spec, row_spec, batch_spec, P(None)) + weight_specs
    out_specs = (batch_spec,) + weight_specs

    def gather(part):
        return lax.all_gather(part, 'shard', axis=0, tiled=True)

    def per_device(x, seg_ids, positions, grad_y, num_tokens, w_q, b_q, w_k, b_k, w_v, b_v, w_o, w_gate, w_up, w_down, norm_attn, norm_mlp):
        tokens, width = x.shape
        ff = w_gate.shape[1]
        half = ff // 2
        q_cols, kv_cols = w_q.shape[1], w_k.shape[1]
        rows = w_q.shape[0]
        down_rows = w_down.shape[0]
        spot = Spot()
        inv_count = 1.0 / num_tokens[0].astype(jnp.float32)

        wqkv = gather(jnp.concatenate([w_q, w_k, w_v], axis=1))
        small_list = [b_q, b_k, b_v, norm_attn, norm_mlp]
        sizes = [v.shape[0] for v in small_list]
        small = lax.all_gather(stack_rows([f32(v)[None, :] for v in small_list]), 'shard', axis=0, tiled=False)
        wo = gather(w_o)
        wg0 = gather(w_gate[:, :half])
        wu0 = gather(w_up[:, :half])
        wdown = gather(w_down)
        wg1 = gather(w_gate[:, half:])
        wu1 = gather(w_up[:, half:])

        cuts = [small[:, i, :n].reshape(-1) for i, n in enumerate(sizes)]
        bias = jnp.concatenate(cuts[:3])
        gain_in, gain_mid = cuts[3], cuts[4]

        cos_t, sin_t = rope_tables(positions)
        start_row = jnp.broadcast_to((jnp.arange(tokens, dtype=jnp.int32) - positions)[None, :], (8, tokens))
        x_f = f32(x)
        inv_in = rms_inverse(x_f)
        normed_in = bf16(x_f * inv_in * gain_in)
        qkv_lin = dot_nn(normed_in, wqkv) + bias
        q_rot, k_rot, v_all, attn_out = attention_fwd(qkv_lin, cos_t, sin_t, start_row)
        resid = bf16(x_f + dot_nn(attn_out, wo))
        resid_f = f32(resid)
        inv_mid = rms_inverse(resid_f)
        normed_mid = bf16(resid_f * inv_mid * gain_mid)

        mid_parts = split_rows(spot, normed_mid, rows)
        o_parts = split_rows(spot, attn_out, rows)
        in_parts = split_rows(spot, normed_in, rows)
        flat_parts = jax.tree.leaves((mid_parts, o_parts, in_parts))

        def swiglu_back(gate_pre, up_proj, d_hid):
            sig_gate = jax.nn.sigmoid(gate_pre)
            act_gate = gate_pre * sig_gate
            d_gate = bf16(d_hid * up_proj * sig_gate * (1.0 + gate_pre * (1.0 - sig_gate)))
            return d_gate, bf16(d_hid * act_gate)

        def down_core(hidden):
            full = dot_tn(hidden, grad_y).reshape(2, 2, down_rows, width)
            return full, swap(bf16(pick(full, 1 - spot.core, 1)), 1)

        def down_x(full, got):
            mine = pick(full, spot.core, 1)
            sent = bf16(pick(mine, 1 - spot.x, 0) + f32(pick(got, 1 - spot.x, 0)))
            return sent, pick(mine, spot.x, 0) + f32(pick(got, spot.x, 0)), swap(sent, 2)

        n_mid, *flat_parts = tie([normed_mid] + flat_parts, [resid])
        mid_parts, o_parts, in_parts = jax.tree.unflatten(jax.tree.structure((mid_parts, o_parts, in_parts)), flat_parts)
        gate_sums = [WeightSum(spot, mid_parts, True, rows) for _ in range(2)]
        up_sums = [WeightSum(spot, mid_parts, False, rows) for _ in range(2)]

        gate0 = dot_nn(n_mid, wg0)
        up0 = dot_nn(n_mid, wu0)
        hidden0 = bf16(gate0 * jax.nn.sigmoid(gate0) * up0)
        hidden0, gate0, up0 = tie([hidden0, gate0, up0], [])
        full0, dgot0 = down_core(hidden0)
        d_hid0 = dot_nt(grad_y, tie([wdown], [full0])[0][:half])
        dg0, du0 = swiglu_back(gate0, up0, round_bf(d_hid0))

        dg0, du0, dgot0, full0 = tie([dg0, du0, dgot0, full0], [])
        dsent0, dkept0, dgot0x = down_x(full0, dgot0)
        c_g0 = gate_sums[0].core(dg0)
        c_u0 = up_sums[0].core(du0)
        dg0, du0, wg0b, wu0b = tie([dg0, du0, wg0, wu0], [c_g0, c_u0, dsent0, dkept0])
        d_mid = dot_nt(dg0, wg0b) + dot_nt(du0, wu0b)
        dg0, du0, got_g, got_u, n_mid = tie([dg0, du0, gate_sums[0].got, up_sums[0].got, n_mid], [d_mid])
        k_g0 = gate_sums[0].first(got_g, dg0)
        k_u0 = up_sums[0].first(got_u, du0)

        n_mid, wd1 = tie([n_mid, wdown], [k_g0, k_u0, gate_sums[0].sent, up_sums[0].sent])
        gate1 = dot_nn(n_mid, wg1)
        d_hid1 = bf16(dot_nt(grad_y, wd1[half:]))
        gate1, d_hid1 = tie([gate1, d_hid1], [])
        n_mid, = tie([n_mid], [gate1, d_hid1])
        up1 = dot_nn(n_mid, wu1)
        hidden1 = bf16(gate1 * jax.nn.sigmoid(gate1) * up1)
        dg1, du1 = swiglu_back(gate1, up1, f32(d_hid1))
        hidden1, dg1, du1, k_g0, k_u0, got_g, got_u = tie([hidden1, dg1, du1, k_g0, k_u0, gate_sums[0].got, up_sums[0].got], [])
        s_g0 = gate_sums[0].second(got_g, k_g0)
        s_u0 = up_sums[0].second(got_u, k_u0)
        hidden1, = tie([hidden1], [s_g0, s_u0])
        full1, dgot1 = down_core(hidden1)
        dg1, du1, full1 = tie([dg1, du1, full1], [])
        c_g1 = gate_sums[1].core(dg1)
        c_u1 = up_sums[1].core(du1)
        full1, dgot1, got_g, got_u = tie([full1, dgot1, gate_sums[0].got, up_sums[0].got], [c_g1, c_u1])
        dsent1, dkept1, dgot1x = down_x(full1, dgot1)
        t_g0 = gate_sums[0].third(got_g, gate_sums[0].kept)
        t_u0 = up_sums[0].third(got_u, up_sums[0].kept)
        dg1, du1, got_g, got_u = tie([dg1, du1, gate_sums[1].got, up_sums[1].got], [dsent1, dkept1, t_g0, t_u0])
        k_u1 = up_sums[1].first(got_u, du1)
        k_g1 = gate_sums[1].first(got_g, dg1)
        dg1, du1, d_mid = tie([dg1, du1, d_mid], [k_g1, k_u1, gate_sums[1].sent, up_sums[1].sent])
        d_mid = d_mid + dot_nt(dg1, wg1)
        d_mid, du1, dkept0, dkept1, dgot0x, dgot1x = tie([d_mid, du1, dkept0, dkept1, dgot0x, dgot1x], [])
        low = spot.y == 0
        down_sent = bf16(jnp.where(low, dkept1 + f32(dgot1x), dkept0 + f32(dgot0x)))
        down_kept = jnp.where(low, dkept0 + f32(dgot0x), dkept1 + f32(dgot1x))
        down_got = swap(down_sent, 4)
        d_mid, du1 = tie([d_mid, du1], [down_sent, down_kept])
        d_mid = round_bf(d_mid + dot_nt(du1, wu1))

        d_resid_norm, sum_norm_mlp = rms_back(d_mid, resid_f, inv_mid, gain_mid)
        d_resid = bf16(f32(grad_y) + d_resid_norm)
        d_resid, k_u1, got_u = tie([d_resid, k_u1, up_sums[1].got], [])
        s_u1 = up_sums[1].second(got_u, k_u1)
        o_cut = width // 2
        o_sums = [WeightSum(spot, o_parts, first, rows) for first in (True, False)]
        c_o = [o_sums[i].core(d_resid[:, i * o_cut:(i + 1) * o_cut]) for i in range(2)]
        d_res_m, = tie([d_resid], c_o + [s_u1])
        d_attn = bf16(dot_nt(d_res_m, wo))
        d_attn, k_g1, got_g, got_o0, got_o1 = tie([d_attn, k_g1, gate_sums[1].got, o_sums[0].got, o_sums[1].got], [])
        s_g1 = gate_sums[1].second(got_g, k_g1)
        k_o = [o_sums[i].first(got, d_resid[:, i * o_cut:(i + 1) * o_cut]) for i, got in enumerate((got_o0, got_o1))]
        d_attn, = tie([d_attn], k_o + [s_g1, o_sums[0].sent, o_sums[1].sent])
        grads_a = attention_bwd(0, q_rot, k_rot, v_all, d_attn, cos_t, sin_t, start_row)
        held = tie(list(grads_a) + k_o + [d_attn, o_sums[0].got, o_sums[1].got, down_got, down_kept, up_sums[1].got], [])
        grads_a, (k_o0, k_o1, d_attn, got_o0, got_o1, down_got, down_kept, got_u) = held[:6], held[6:]
        down_mine = bf16(down_kept + f32(down_got))
        down_rep = swap_rep(down_mine)
        t_u1 = up_sums[1].third(got_u, up_sums[1].kept)
        s_o = [o_sums[0].second(got_o0, k_o0), o_sums[1].second(got_o1, k_o1)]
        d_attn, = tie([d_attn], s_o + [down_mine, t_u1])
        grads_b = attention_bwd(1, q_rot, k_rot, v_all, d_attn, cos_t, sin_t, start_row)
        d_qkv = jnp.concatenate([grads_a[0], grads_b[0], grads_a[1], grads_b[1], grads_a[2], grads_b[2]], axis=1)
        sum_bq, sum_bk, sum_bv = [jnp.concatenate([grads_a[i][0], grads_b[i][0]]) for i in (3, 4, 5)]
        d_qkv, got_g, got_o0, got_o1 = tie([d_qkv, gate_sums[1].got, o_sums[0].got, o_sums[1].got], [])
        q_cut = d_qkv.shape[1] // 2
        q_sums = [WeightSum(spot, in_parts, first, rows) for first in (True, False)]
        c_q = [q_sums[i].core(d_qkv[:, i * q_cut:(i + 1) * q_cut]) for i in range(2)]
        t_g1 = gate_sums[1].third(got_g, gate_sums[1].kept)
        t_o = [o_sums[0].third(got_o0, o_sums[0].kept), o_sums[1].third(got_o1, o_sums[1].kept)]
        d_qkv, got_q0, got_q1 = tie([d_qkv, q_sums[0].got, q_sums[1].got], c_q + t_o + [t_g1])
        k_q = [q_sums[i].first(got, d_qkv[:, i * q_cut:(i + 1) * q_cut]) for i, got in enumerate((got_q0, got_q1))]
        d_qkv, = tie([d_qkv], k_q + [q_sums[0].sent, q_sums[1].sent])
        d_normed_in = round_bf(dot_nt(d_qkv, wqkv))
        d_x_norm, sum_norm_attn = rms_back(d_normed_in, x_f, inv_in, gain_in)
        sum_norm_attn, = tie([sum_norm_attn], [])
        k_q0, k_q1, got_q0, got_q1 = tie(k_q + [q_sums[0].got, q_sums[1].got], [sum_norm_attn])
        s_q = [q_sums[0].second(got_q0, k_q0), q_sums[1].second(got_q1, k_q1)]
        d_resid, d_x_norm = tie([d_resid, d_x_norm], s_q)
        grad_x = bf16(f32(d_resid) + d_x_norm)

        vecs = [sum_bq, sum_bk, sum_bv, sum_norm_attn, sum_norm_mlp]
        flat = stack_rows([v.reshape(8, 1, -1) for v in vecs])
        flat = lax.psum(flat, ('rep', 'shard'))
        t_q = [part.third(part.got, part.kept) for part in q_sums]
        late = [gate_sums[1], up_sums[1]] + o_sums
        ends = tie([part.got for part in late] + [down_rep, flat], t_q)
        for part, got in zip(late, ends):
            part.got = got
        down_rep, flat = ends[-2:]
        flat = pick(flat, lax.axis_index('shard'), 0) * inv_count
        vec_out = [flat[i, :n] for i, n in enumerate(sizes)]

        def joined(parts):
            return jnp.concatenate([part.result() for part in parts], axis=1) * inv_count

        qkv_sum = joined(q_sums)
        return (grad_x, qkv_sum[:, :q_cols], vec_out[0], qkv_sum[:, q_cols:q_cols + kv_cols], vec_out[1], qkv_sum[:, q_cols + kv_cols:], vec_out[2], joined(o_sums),
                joined(gate_sums), joined(up_sums), (f32(down_mine) + f32(down_rep)) * inv_count, vec_out[3], vec_out[4])

    return jax.shard_map(per_device, mesh=mesh, in_specs=in_specs, out_specs=out_specs, check_vma=False)
```

```python
import jax
import jax.numpy as jnp
from jax import lax
from jax.experimental import pallas as pl
from jax.experimental.pallas import tpu as pltpu
from jax.sharding import PartitionSpec as P


HEAD_DIM = 128
HEADS = 12
KV_HEADS = 2
GROUP = HEADS // KV_HEADS
ROPE_THETA = 1000000.0
EPS = 1e-6
QB = 256
SCALE = HEAD_DIM ** -0.5
LOG2E = 1.4426950408889634


def rope_tables(positions):
    half_dim = HEAD_DIM // 2
    inv_freq = ROPE_THETA ** (-2.0 * jnp.arange(half_dim, dtype=jnp.float32) / HEAD_DIM)
    angle = positions.astype(jnp.float32)[:, None] * inv_freq[None, :]
    cos_t = jnp.cos(angle)
    sin_t = jnp.sin(angle)
    return jnp.concatenate([cos_t, cos_t], axis=-1), jnp.concatenate([-sin_t, sin_t], axis=-1)


def dot_nn(a, b):
    return lax.dot_general(a, b, (((1,), (0,)), ((), ())), preferred_element_type=jnp.float32)


def dot_nt(a, b):
    return lax.dot_general(a, b, (((1,), (1,)), ((), ())), preferred_element_type=jnp.float32)


def dot_tn(a, b):
    return lax.dot_general(a, b, (((0,), (0,)), ((), ())), preferred_element_type=jnp.float32)


def round_bf(vals):
    return lax.reduce_precision(vals, 8, 7)


def exp_scores(k_part, q_blk, first_row, start_row):
    s_t = dot_nt(k_part, q_blk)
    key_idx = lax.broadcasted_iota(jnp.int32, (QB, QB), 0)
    row_idx = lax.broadcasted_iota(jnp.int32, (QB, QB), 1)
    parts = []
    for base in range(0, first_row, QB):
        parts.append(jnp.where(key_idx >= start_row - base, s_t[base:base + QB], -1e30))
    parts.append(jnp.where((key_idx >= start_row - first_row) & (key_idx <= row_idx), s_t[first_row:], -1e30))
    s_t = jnp.concatenate(parts, axis=0)
    e_t = jnp.exp2((s_t - jnp.max(s_t, axis=0, keepdims=True)) * (SCALE * LOG2E))
    return e_t, 1.0 / jnp.sum(e_t, axis=0, keepdims=True)


def attn_fwd_kernel(q_in, k_in, v_in, cos_ref, sin_ref, start_ref, q_out, k_out, v_out, o_out, vt_scr):
    tokens = q_in.shape[0]

    @pl.when(pl.program_id(0) % GROUP == 0)
    def _():
        k_f = k_in[...]
        k_out[...] = (k_f * cos_ref[...] + pltpu.roll(k_f, HEAD_DIM // 2, 1) * sin_ref[...]).astype(jnp.bfloat16)
        v_f = v_in[...]
        v_out[...] = v_f.astype(jnp.bfloat16)
        vt_scr[...] = v_f.T.astype(jnp.bfloat16)

    q_f = q_in[...]
    q_out[...] = (q_f * cos_ref[...] + pltpu.roll(q_f, HEAD_DIM // 2, 1) * sin_ref[...]).astype(jnp.bfloat16)
    for first in range(0, tokens, QB):
        keys = first + QB
        e_t, inv_sum = exp_scores(k_out[:keys, :], q_out[first:keys, :], first, start_ref[0:1, first:keys])
        p_t = (e_t * inv_sum).astype(jnp.bfloat16)
        o_t = dot_nn(vt_scr[:, :keys], p_t)
        o_out[first:keys, :] = o_t.T.astype(jnp.bfloat16)


def column_sums(vals):
    return jnp.broadcast_to(jnp.sum(vals, axis=0, keepdims=True), (8, vals.shape[1]))


def attn_bwd_kernel(q_ref, k_ref, v_ref, do_ref, cos_ref, sin_ref, start_ref, dq_out, dk_out, dv_out, bq_out, bk_out, bv_out, dk_acc, dv_acc, kt_scr, dq_scr):
    tokens = q_ref.shape[0]
    step = pl.program_id(0) % GROUP

    @pl.when(step == 0)
    def _():
        kt_scr[...] = k_ref[...].astype(jnp.float32).T.astype(jnp.bfloat16)
        dk_acc[...] = jnp.zeros_like(dk_acc)
        dv_acc[...] = jnp.zeros_like(dv_acc)

    for first in range(0, tokens, QB):
        keys = first + QB
        q_blk = q_ref[first:keys, :]
        do_blk = do_ref[first:keys, :]
        e_t, inv_sum = exp_scores(k_ref[:keys, :], q_blk, first, start_ref[0:1, first:keys])
        p_t = e_t * inv_sum
        dp_t = dot_nt(v_ref[:keys, :], do_blk)
        dv_acc[:keys, :] += dot_nn(p_t.astype(jnp.bfloat16), do_blk)
        delta = jnp.sum(p_t * dp_t, axis=0, keepdims=True)
        ds_t = (p_t * (dp_t - delta) * SCALE).astype(jnp.bfloat16)
        dk_acc[:keys, :] += dot_nn(ds_t, q_blk)
        dq_scr[first:keys, :] = dot_nn(kt_scr[:, :keys], ds_t).T

    def rope_back(grad):
        grad = grad.astype(jnp.bfloat16).astype(jnp.float32)
        return grad * cos_ref[...] - pltpu.roll(grad, HEAD_DIM // 2, 1) * sin_ref[...]

    dq_lin = rope_back(dq_scr[...])
    dq_out[...] = dq_lin.astype(jnp.bfloat16)
    bq_out[...] = column_sums(dq_lin)

    @pl.when(step == GROUP - 1)
    def _():
        dk_lin = rope_back(dk_acc[...])
        dk_out[...] = dk_lin.astype(jnp.bfloat16)
        bk_out[...] = column_sums(dk_lin)
        dv_bf = dv_acc[...].astype(jnp.bfloat16)
        dv_out[...] = dv_bf
        bv_out[...] = column_sums(dv_bf.astype(jnp.float32))


def head_spec(tokens, base):
    return pl.BlockSpec((tokens, HEAD_DIM), lambda h: (0, base + h))


def kv_spec(tokens, base):
    return pl.BlockSpec((tokens, HEAD_DIM), lambda h: (0, base + h // GROUP))


def whole_spec(shape):
    return pl.BlockSpec(shape, lambda h: (0, 0))


def attention_fwd(qkv_lin, cos_t, sin_t, start_row):
    tokens = qkv_lin.shape[0]
    table = whole_spec((tokens, HEAD_DIM))
    pairs = HEADS * tokens * tokens * 0.6
    return pl.pallas_call(
        attn_fwd_kernel,
        grid=(HEADS,),
        in_specs=[head_spec(tokens, 0), kv_spec(tokens, HEADS), kv_spec(tokens, HEADS + KV_HEADS), table, table, whole_spec((8, tokens))],
        out_specs=[head_spec(tokens, 0), kv_spec(tokens, 0), kv_spec(tokens, 0), head_spec(tokens, 0)],
        out_shape=[
            jax.ShapeDtypeStruct((tokens, HEADS * HEAD_DIM), jnp.bfloat16),
            jax.ShapeDtypeStruct((tokens, KV_HEADS * HEAD_DIM), jnp.bfloat16),
            jax.ShapeDtypeStruct((tokens, KV_HEADS * HEAD_DIM), jnp.bfloat16),
            jax.ShapeDtypeStruct((tokens, HEADS * HEAD_DIM), jnp.bfloat16),
        ],
        scratch_shapes=[pltpu.VMEM((HEAD_DIM, tokens), jnp.bfloat16)],
        compiler_params=pltpu.CompilerParams(dimension_semantics=("arbitrary",), vmem_limit_bytes=48 * 1024 * 1024),
        cost_estimate=pl.CostEstimate(flops=int(pairs * 128 * 16), bytes_accessed=30000000, transcendentals=int(pairs)),
        name="attn_fwd",
    )(qkv_lin, qkv_lin, qkv_lin, cos_t, sin_t, start_row)


def attention_bwd(kv_head, q_rot, k_rot, v_all, d_out, cos_t, sin_t, start_row):
    tokens = q_rot.shape[0]
    table = whole_spec((tokens, HEAD_DIM))
    pairs = GROUP * tokens * tokens * 0.6
    q_in = head_spec(tokens, kv_head * GROUP)
    kv_in = pl.BlockSpec((tokens, HEAD_DIM), lambda h: (0, kv_head))
    row_q = pl.BlockSpec((8, HEAD_DIM), lambda h: (0, h))
    acc = pltpu.VMEM((tokens, HEAD_DIM), jnp.float32)
    q_cols = GROUP * HEAD_DIM
    return pl.pallas_call(
        attn_bwd_kernel,
        grid=(GROUP,),
        in_specs=[q_in, kv_in, kv_in, q_in, table, table, whole_spec((8, tokens))],
        out_specs=[head_spec(tokens, 0), table, table, row_q, whole_spec((8, HEAD_DIM)), whole_spec((8, HEAD_DIM))],
        out_shape=[
            jax.ShapeDtypeStruct((tokens, q_cols), jnp.bfloat16),
            jax.ShapeDtypeStruct((tokens, HEAD_DIM), jnp.bfloat16),
            jax.ShapeDtypeStruct((tokens, HEAD_DIM), jnp.bfloat16),
            jax.ShapeDtypeStruct((8, q_cols), jnp.float32),
            jax.ShapeDtypeStruct((8, HEAD_DIM), jnp.float32),
            jax.ShapeDtypeStruct((8, HEAD_DIM), jnp.float32),
        ],
        scratch_shapes=[acc, acc, pltpu.VMEM((HEAD_DIM, tokens), jnp.bfloat16), acc],
        compiler_params=pltpu.CompilerParams(dimension_semantics=("arbitrary",), vmem_limit_bytes=48 * 1024 * 1024),
        cost_estimate=pl.CostEstimate(flops=int(pairs * 128 * 30), bytes_accessed=15000000, transcendentals=int(pairs)),
        name="attn_bwd",
    )(q_rot, k_rot, v_all, d_out, cos_t, sin_t, start_row)


def rms_inverse(vals):
    return lax.rsqrt(jnp.mean(vals * vals, axis=-1, keepdims=True) + EPS)


def rms_back(d_normed, vals, inv_rms, gain):
    d_scaled = d_normed * gain
    d_vals = inv_rms * d_scaled - vals * (inv_rms ** 3) * jnp.mean(d_scaled * vals, axis=-1, keepdims=True)
    return d_vals, jnp.sum(d_normed * vals * inv_rms, axis=0)


def pick(arr, index, axis):
    return lax.dynamic_index_in_dim(arr, index, axis, keepdims=False)


def swap(arr, bit):
    return lax.ppermute(arr, 'shard', [(s, s ^ bit) for s in range(8)])


def swap_rep(arr):
    return lax.ppermute(arr, 'rep', [(0, 1), (1, 0)])


def f32(arr):
    return arr.astype(jnp.float32)


def bf16(arr):
    return arr.astype(jnp.bfloat16)


def stack_rows(vecs):
    rows = [jnp.pad(v, [(0, 0)] * (v.ndim - 1) + [(0, 256 - v.shape[-1])]) for v in vecs]
    rows = jnp.concatenate(rows, axis=-2)
    return jnp.pad(rows, [(0, 0)] * (rows.ndim - 2) + [(0, 8 - len(vecs)), (0, 0)])


class Spot:
    def __init__(self):
        shard = lax.axis_index('shard')
        self.core = shard % 2
        self.x = (shard // 2) % 2
        self.y = shard // 4


def split_rows(spot, acts, rows):
    tokens = acts.shape[0]
    cut = acts.T.reshape(2, 2, 2, rows, tokens)
    out = []
    for axis, here in ((1, spot.x), (0, spot.y)):
        pair = []
        for core in (1 - spot.core, spot.core):
            mine = pick(cut, core, 2)
            pair.append(jnp.stack([pick(mine, 1 - here, axis), pick(mine, here, axis)]).reshape(4 * rows, tokens))
        out.append(tuple(pair))
    return tuple(out)


def tie(now, after):
    out = lax.optimization_barrier((tuple(now), tuple(after)))
    return out[0]


class WeightSum:
    def __init__(self, spot, parts, x_first, rows):
        self.spot, self.x_first, self.rows = spot, x_first, rows
        self.to_core, self.own_acts = parts[0] if x_first else parts[1]
        self.bit = 2 if x_first else 4
        self.here2, self.bit2 = (spot.y, 4) if x_first else (spot.x, 2)

    def core(self, grads):
        self.sent = bf16(dot_nn(self.to_core, grads))
        self.got = swap(self.sent, 1)
        return self.sent

    def first(self, got, grads):
        own, = tie([dot_nn(self.own_acts, grads) + f32(got)], [])
        self.sent = bf16(own[:2 * self.rows])
        self.got = swap(self.sent, self.bit)
        return own

    def second(self, got, kept):
        cols = got.shape[1]
        got = got.reshape(2, self.rows, cols)
        kept = kept[2 * self.rows:].reshape(2, self.rows, cols)
        self.sent = bf16(pick(kept, 1 - self.here2, 0) + f32(pick(got, 1 - self.here2, 0)))
        self.got = swap(self.sent, self.bit2)
        self.kept = pick(kept, self.here2, 0) + f32(pick(got, self.here2, 0))
        return self.sent

    def third(self, got, kept):
        self.sent = bf16(kept + f32(got))
        self.got = swap_rep(self.sent)
        return self.sent

    def result(self):
        return f32(self.sent) + f32(self.got)


def solution(mesh):
    batch_spec = P(('rep', 'shard'), None)
    row_spec = P(('rep', 'shard'))
    mat_spec = P('shard', None)
    vec_spec = P('shard')
    weight_specs = (mat_spec, vec_spec, mat_spec, vec_spec, mat_spec, vec_spec, mat_spec, mat_spec, mat_spec, mat_spec, vec_spec, vec_spec)
    in_specs = (batch_spec, row_spec, row_spec, batch_spec, P(None)) + weight_specs
    out_specs = (batch_spec,) + weight_specs

    def gather(part):
        return lax.all_gather(part, 'shard', axis=0, tiled=True)

    def per_device(x, seg_ids, positions, grad_y, num_tokens, w_q, b_q, w_k, b_k, w_v, b_v, w_o, w_gate, w_up, w_down, norm_attn, norm_mlp):
        tokens, width = x.shape
        ff = w_gate.shape[1]
        half = ff // 2
        q_cols, kv_cols = w_q.shape[1], w_k.shape[1]
        rows = w_q.shape[0]
        down_rows = w_down.shape[0]
        spot = Spot()
        inv_count = 1.0 / num_tokens[0].astype(jnp.float32)

        wqkv = gather(jnp.concatenate([w_q, w_k, w_v], axis=1))
        small_list = [b_q, b_k, b_v, norm_attn, norm_mlp]
        sizes = [v.shape[0] for v in small_list]
        small = lax.all_gather(stack_rows([f32(v)[None, :] for v in small_list]), 'shard', axis=0, tiled=False)
        wo = gather(w_o)
        wg0 = gather(w_gate[:, :half])
        wu0 = gather(w_up[:, :half])
        wdown = gather(w_down)
        wg1 = gather(w_gate[:, half:])
        wu1 = gather(w_up[:, half:])

        cuts = [small[:, i, :n].reshape(-1) for i, n in enumerate(sizes)]
        bias = jnp.concatenate(cuts[:3])
        gain_in, gain_mid = cuts[3], cuts[4]

        cos_t, sin_t = rope_tables(positions)
        start_row = jnp.broadcast_to((jnp.arange(tokens, dtype=jnp.int32) - positions)[None, :], (8, tokens))
        x_f = f32(x)
        inv_in = rms_inverse(x_f)
        normed_in = bf16(x_f * inv_in * gain_in)
        qkv_lin = dot_nn(normed_in, wqkv) + bias
        q_rot, k_rot, v_all, attn_out = attention_fwd(qkv_lin, cos_t, sin_t, start_row)
        resid = bf16(x_f + dot_nn(attn_out, wo))
        resid_f = f32(resid)
        inv_mid = rms_inverse(resid_f)
        normed_mid = bf16(resid_f * inv_mid * gain_mid)

        mid_parts = split_rows(spot, normed_mid, rows)
        o_parts = split_rows(spot, attn_out, rows)
        in_parts = split_rows(spot, normed_in, rows)
        flat_parts = jax.tree.leaves((mid_parts, o_parts, in_parts))

        def swiglu_back(gate_pre, up_proj, d_hid):
            sig_gate = jax.nn.sigmoid(gate_pre)
            act_gate = gate_pre * sig_gate
            d_gate = bf16(d_hid * up_proj * sig_gate * (1.0 + gate_pre * (1.0 - sig_gate)))
            return d_gate, bf16(d_hid * act_gate)

        def down_core(hidden):
            full = dot_tn(hidden, grad_y).reshape(2, 2, down_rows, width)
            return full, swap(bf16(pick(full, 1 - spot.core, 1)), 1)

        def down_x(full, got):
            mine = pick(full, spot.core, 1)
            sent = bf16(pick(mine, 1 - spot.x, 0) + f32(pick(got, 1 - spot.x, 0)))
            return sent, pick(mine, spot.x, 0) + f32(pick(got, spot.x, 0)), swap(sent, 2)

        n_mid, *flat_parts = tie([normed_mid] + flat_parts, [resid])
        mid_parts, o_parts, in_parts = jax.tree.unflatten(jax.tree.structure((mid_parts, o_parts, in_parts)), flat_parts)
        gate_sums = [WeightSum(spot, mid_parts, True, rows) for _ in range(2)]
        up_sums = [WeightSum(spot, mid_parts, False, rows) for _ in range(2)]

        gate0 = dot_nn(n_mid, wg0)
        up0 = dot_nn(n_mid, wu0)
        hidden0 = bf16(gate0 * jax.nn.sigmoid(gate0) * up0)
        hidden0, gate0, up0 = tie([hidden0, gate0, up0], [])
        full0, dgot0 = down_core(hidden0)
        d_hid0 = dot_nt(grad_y, tie([wdown], [full0])[0][:half])
        dg0, du0 = swiglu_back(gate0, up0, round_bf(d_hid0))

        dg0, du0, dgot0, full0 = tie([dg0, du0, dgot0, full0], [])
        dsent0, dkept0, dgot0x = down_x(full0, dgot0)
        c_g0 = gate_sums[0].core(dg0)
        c_u0 = up_sums[0].core(du0)
        dg0, du0, wg0b, wu0b = tie([dg0, du0, wg0, wu0], [c_g0, c_u0, dsent0, dkept0])
        d_mid = dot_nt(dg0, wg0b) + dot_nt(du0, wu0b)
        dg0, du0, got_g, got_u, n_mid = tie([dg0, du0, gate_sums[0].got, up_sums[0].got, n_mid], [d_mid])
        k_g0 = gate_sums[0].first(got_g, dg0)
        k_u0 = up_sums[0].first(got_u, du0)

        n_mid, wd1 = tie([n_mid, wdown], [k_g0, k_u0, gate_sums[0].sent, up_sums[0].sent])
        gate1 = dot_nn(n_mid, wg1)
        d_hid1 = bf16(dot_nt(grad_y, wd1[half:]))
        gate1, d_hid1 = tie([gate1, d_hid1], [])
        n_mid, = tie([n_mid], [gate1, d_hid1])
        up1 = dot_nn(n_mid, wu1)
        hidden1 = bf16(gate1 * jax.nn.sigmoid(gate1) * up1)
        dg1, du1 = swiglu_back(gate1, up1, f32(d_hid1))
        hidden1, dg1, du1, k_g0, k_u0, got_g, got_u = tie([hidden1, dg1, du1, k_g0, k_u0, gate_sums[0].got, up_sums[0].got], [])
        s_g0 = gate_sums[0].second(got_g, k_g0)
        s_u0 = up_sums[0].second(got_u, k_u0)
        hidden1, = tie([hidden1], [s_g0, s_u0])
        full1, dgot1 = down_core(hidden1)
        dg1, du1, full1 = tie([dg1, du1, full1], [])
        c_g1 = gate_sums[1].core(dg1)
        c_u1 = up_sums[1].core(du1)
        full1, dgot1 = tie([full1, dgot1], [c_g1, c_u1])
        dsent1, dkept1, dgot1x = down_x(full1, dgot1)
        dg1, du1, got_g, got_u = tie([dg1, du1, gate_sums[1].got, up_sums[1].got], [dsent1, dkept1])
        k_u1 = up_sums[1].first(got_u, du1)
        k_g1 = gate_sums[1].first(got_g, dg1)
        dg1, du1, d_mid, got_g, got_u = tie([dg1, du1, d_mid, gate_sums[0].got, up_sums[0].got], [k_g1, k_u1, gate_sums[1].sent, up_sums[1].sent])
        t_g0 = gate_sums[0].third(got_g, gate_sums[0].kept)
        t_u0 = up_sums[0].third(got_u, up_sums[0].kept)
        d_mid, = tie([d_mid], [t_g0, t_u0])
        d_mid = d_mid + dot_nt(dg1, wg1)
        d_mid, du1, dkept0, dkept1, dgot0x, dgot1x = tie([d_mid, du1, dkept0, dkept1, dgot0x, dgot1x], [])
        low = spot.y == 0
        down_sent = bf16(jnp.where(low, dkept1 + f32(dgot1x), dkept0 + f32(dgot0x)))
        down_kept = jnp.where(low, dkept0 + f32(dgot0x), dkept1 + f32(dgot1x))
        down_got = swap(down_sent, 4)
        d_mid, du1 = tie([d_mid, du1], [down_sent, down_kept])
        d_mid = round_bf(d_mid + dot_nt(du1, wu1))

        d_resid_norm, sum_norm_mlp = rms_back(d_mid, resid_f, inv_mid, gain_mid)
        d_resid = bf16(f32(grad_y) + d_resid_norm)
        d_resid, k_u1, got_u = tie([d_resid, k_u1, up_sums[1].got], [])
        s_u1 = up_sums[1].second(got_u, k_u1)
        o_cut = width // 2
        o_sums = [WeightSum(spot, o_parts, first, rows) for first in (True, False)]
        c_o = [o_sums[i].core(d_resid[:, i * o_cut:(i + 1) * o_cut]) for i in range(2)]
        d_res_m, = tie([d_resid], c_o + [s_u1])
        d_attn = bf16(dot_nt(d_res_m, wo))
        d_attn, k_g1, got_g, got_o0, got_o1 = tie([d_attn, k_g1, gate_sums[1].got, o_sums[0].got, o_sums[1].got], [])
        s_g1 = gate_sums[1].second(got_g, k_g1)
        k_o = [o_sums[i].first(got, d_resid[:, i * o_cut:(i + 1) * o_cut]) for i, got in enumerate((got_o0, got_o1))]
        d_attn, = tie([d_attn], k_o + [s_g1, o_sums[0].sent, o_sums[1].sent])
        grads_a = attention_bwd(0, q_rot, k_rot, v_all, d_attn, cos_t, sin_t, start_row)
        held = tie(list(grads_a) + k_o + [d_attn, o_sums[0].got, o_sums[1].got, down_got, down_kept, up_sums[1].got], [])
        grads_a, (k_o0, k_o1, d_attn, got_o0, got_o1, down_got, down_kept, got_u) = held[:6], held[6:]
        down_mine = bf16(down_kept + f32(down_got))
        down_rep = swap_rep(down_mine)
        t_u1 = up_sums[1].third(got_u, up_sums[1].kept)
        s_o = [o_sums[0].second(got_o0, k_o0), o_sums[1].second(got_o1, k_o1)]
        d_attn, = tie([d_attn], s_o + [down_mine, t_u1])
        grads_b = attention_bwd(1, q_rot, k_rot, v_all, d_attn, cos_t, sin_t, start_row)
        d_qkv = jnp.concatenate([grads_a[0], grads_b[0], grads_a[1], grads_b[1], grads_a[2], grads_b[2]], axis=1)
        sum_bq, sum_bk, sum_bv = [jnp.concatenate([grads_a[i][0], grads_b[i][0]]) for i in (3, 4, 5)]
        d_qkv, got_g, got_o0, got_o1 = tie([d_qkv, gate_sums[1].got, o_sums[0].got, o_sums[1].got], [])
        q_cut = d_qkv.shape[1] // 2
        q_sums = [WeightSum(spot, in_parts, first, rows) for first in (True, False)]
        c_q = [q_sums[i].core(d_qkv[:, i * q_cut:(i + 1) * q_cut]) for i in range(2)]
        t_g1 = gate_sums[1].third(got_g, gate_sums[1].kept)
        t_o = [o_sums[0].third(got_o0, o_sums[0].kept), o_sums[1].third(got_o1, o_sums[1].kept)]
        d_qkv, got_q0, got_q1 = tie([d_qkv, q_sums[0].got, q_sums[1].got], c_q + t_o + [t_g1])
        k_q = [q_sums[i].first(got, d_qkv[:, i * q_cut:(i + 1) * q_cut]) for i, got in enumerate((got_q0, got_q1))]
        d_qkv, = tie([d_qkv], k_q + [q_sums[0].sent, q_sums[1].sent])
        d_normed_in = round_bf(dot_nt(d_qkv, wqkv))
        d_x_norm, sum_norm_attn = rms_back(d_normed_in, x_f, inv_in, gain_in)
        sum_norm_attn, = tie([sum_norm_attn], [])
        k_q0, k_q1, got_q0, got_q1 = tie(k_q + [q_sums[0].got, q_sums[1].got], [sum_norm_attn])
        s_q = [q_sums[0].second(got_q0, k_q0), q_sums[1].second(got_q1, k_q1)]
        d_resid, d_x_norm = tie([d_resid, d_x_norm], s_q)
        grad_x = bf16(f32(d_resid) + d_x_norm)

        vecs = [sum_bq, sum_bk, sum_bv, sum_norm_attn, sum_norm_mlp]
        flat = stack_rows([v.reshape(8, 1, -1) for v in vecs])
        flat = lax.psum(flat, ('rep', 'shard'))
        t_q = [part.third(part.got, part.kept) for part in q_sums]
        late = gate_sums + up_sums + o_sums
        ends = tie([part.got for part in late] + [down_rep, flat], t_q)
        for part, got in zip(late, ends):
            part.got = got
        down_rep, flat = ends[-2:]
        flat = pick(flat, lax.axis_index('shard'), 0) * inv_count
        vec_out = [flat[i, :n] for i, n in enumerate(sizes)]

        def joined(parts):
            return jnp.concatenate([part.result() for part in parts], axis=1) * inv_count

        qkv_sum = joined(q_sums)
        return (grad_x, qkv_sum[:, :q_cols], vec_out[0], qkv_sum[:, q_cols:q_cols + kv_cols], vec_out[1], qkv_sum[:, q_cols + kv_cols:], vec_out[2], joined(o_sums),
                joined(gate_sums), joined(up_sums), (f32(down_mine) + f32(down_rep)) * inv_count, vec_out[3], vec_out[4])

    return jax.shard_map(per_device, mesh=mesh, in_specs=in_specs, out_specs=out_specs, check_vma=False)
```
